32 devices in a mesh: gx: 2 (over y), gy: 4 (over z), gz: 4 (over x, core).
Axes of the slice: x: 2, y: 2, z: 4, core: 2. Of those that a mesh axis runs over, the one named last changes fastest.
Arguments:
- density: float32 [64, 64, 512], P('gx', 'gy', 'gz'), may hold values from -8 to 8
Outputs:
- potential: float32 [64, 64, 512], P('gx', 'gy', 'gz')
The draws below stay inside these ranges and needn't reach their ends.
All inputs are finite; a program needn't handle non-finite values.
Results may differ from the reference program's by a relative error of at most 0.00002.
Values sent between devices are 32-bit elements; how exact they have to be, the bound alone decides.
A program may use at most 128 MiB of HBM per device.

```python
import jax
import jax.numpy as jnp
from jax import lax

LEVELS = 7
CSWEEPS = 4
NX = 64
NY = 64
NZ = 512


def rough_field(key, shape):
    return jnp.clip(jax.random.normal(key, shape, jnp.float32), -4.0, 4.0)


def draw_density(key, part):
    first_key = jax.random.fold_in(key, 21)
    second_key = jax.random.fold_in(key, 22)
    shape = (NX, NY, NZ)
    first = rough_field(first_key, shape)
    second = rough_field(second_key, shape)
    beside_all = jnp.zeros(shape, jnp.float32)
    for which in range(3):
        beside_all = beside_all + jnp.roll(first, 1, which) + jnp.roll(first, -1, which)
    sharp = 6.0 * first - beside_all
    total = 0.4 * sharp + 0.4 * second
    return jnp.clip(total, -8.0, 8.0).astype(jnp.float32)


def setup_inputs(seed: int = 0) -> dict:
    key_of = jax.random.split(jax.random.key(seed), 2)
    density = draw_density(jax.random.fold_in(key_of[1], 71), 0)
    return dict(density=density)


rsd_beta = 0.5
centre = 4.0 + 2.0 * (1.0 + rsd_beta)


def stencil_sum(padded):
    plane = padded[2:, 1:-1, 1:-1] + padded[:-2, 1:-1, 1:-1] + padded[1:-1, 2:, 1:-1] + padded[1:-1, :-2, 1:-1]
    sight = padded[1:-1, 1:-1, 2:] + padded[1:-1, 1:-1, :-2]
    return plane + (1.0 + rsd_beta) * sight


def parity_of(shape):
    total = lax.broadcasted_iota(jnp.int32, shape, 0) + lax.broadcasted_iota(jnp.int32, shape, 1)
    total = total + lax.broadcasted_iota(jnp.int32, shape, 2)
    return total % 2


def half_sweep(field, source, scale, chosen):
    update = (source / scale + stencil_sum(jnp.pad(field, 1))) / centre
    return jnp.where(chosen, update, field)


def full_sweep(field, source, scale, parity):
    field = half_sweep(field, source, scale, parity == 0)
    return half_sweep(field, source, scale, parity == 1)


def restrict(residue):
    shape = residue.shape
    blocks = residue.reshape(shape[0] // 2, 2, shape[1] // 2, 2, shape[2] // 2, 2)
    return jnp.mean(blocks, axis=(1, 3, 5))


def prolong(coarse):
    return jnp.repeat(jnp.repeat(jnp.repeat(coarse, 2, 0), 2, 1), 2, 2)


def local_cycle(source, level):
    scale = 0.25 ** level
    parity = parity_of(source.shape)
    field = jnp.zeros_like(source)
    if level == LEVELS - 1:
        for number in range(CSWEEPS):
            field = full_sweep(field, source, scale, parity)
        return field
    for number in range(2):
        field = full_sweep(field, source, scale, parity)
    residue = source - scale * (centre * field - stencil_sum(jnp.pad(field, 1)))
    field = field + prolong(local_cycle(restrict(residue), level + 1))
    for number in range(2):
        field = full_sweep(field, source, scale, parity)
    return field


def reference(density):
    return local_cycle(density, 0)
```

```python
import functools

import jax
import jax.numpy as jnp
from jax import lax
from jax.experimental import pallas as pl
from jax.experimental.pallas import tpu as pltpu
from jax.sharding import PartitionSpec as P

LEVELS = 7
CSWEEPS = 4
rsd_beta = 0.5
centre = 4.0 + 2.0 * (1.0 + rsd_beta)
along = 1.0 + rsd_beta
inverse = 1.0 / centre
F32 = jnp.float32
LANES = 128
AXES = ("gx", "gy", "gz")
STEPS_XY = [(dx, dy) for dx in (-1, 0, 1) for dy in (-1, 0, 1) if (dx, dy) != (0, 0)]


def up_to(value, unit):
    return -(-value // unit) * unit


class Split:
    def __init__(self, block, margins, counts):
        self.block, self.margins, self.counts = block, margins, counts
        self.planes = block[0] + 2 * margins[0]
        self.rows = up_to(block[1] + 2 * margins[1], 8)
        self.lanes = up_to(block[2] + 2 * margins[2], LANES)
        self.per = LANES // margins[2]
        self.packs = -(-self.planes // self.per)
        self.shape = (self.planes, self.rows, self.lanes)

    def scratch(self):
        land_x = (2, self.margins[0], self.block[1], LANES)
        land_y = (2, self.planes, self.margins[1], LANES)
        stage_y = (2, self.block[0], self.margins[1], LANES)
        packed = (2, self.packs, self.rows, LANES)
        one = [
            pltpu.VMEM(land_x, F32),
            pltpu.VMEM(land_x, F32),
            pltpu.VMEM(land_y, F32),
            pltpu.VMEM(stage_y, F32),
            pltpu.VMEM(packed, F32),
            pltpu.VMEM(packed, F32),
            pltpu.SemaphoreType.DMA((10,)),
            pltpu.SemaphoreType.DMA((10,)),
        ]
        own = [
            pltpu.VMEM(self.shape, F32),
            pltpu.VMEM((self.planes + 2,) + self.shape[1:], F32),
            pltpu.VMEM((2,) + self.shape[1:], jnp.int32),
        ]
        return own, one, list(one)


class Whole:
    def __init__(self, size):
        self.size = size
        self.rows = up_to(size[1], 8)
        self.lanes = up_to(size[2], LANES)
        self.shape = (size[0], self.rows, self.lanes)

    def scratch(self):
        return [
            pltpu.VMEM(self.shape, F32),
            pltpu.VMEM((self.shape[0] + 2,) + self.shape[1:], F32),
        ]


def iota(shape, dim):
    return lax.broadcasted_iota(jnp.int32, shape, dim)


def dot(a, b):
    return jnp.dot(a, b, precision=lax.Precision.HIGHEST, preferred_element_type=F32)


def local_of(index, length, margin, total):
    return jnp.where(index < total - margin, index, index - total)


def beside_sum(below, here, above, size, rows, lanes):
    down, up = pltpu.roll(here, 1, 0), pltpu.roll(here, rows - 1, 0)
    left, right = pltpu.roll(here, 1, 1), pltpu.roll(here, lanes - 1, 1)
    if size is not None:
        if size[1] == rows:
            row = iota(here.shape, 0)
            down = jnp.where(row == 0, 0.0, down)
            up = jnp.where(row == rows - 1, 0.0, up)
        if size[2] == lanes:
            lane = iota(here.shape, 1)
            left = jnp.where(lane == 0, 0.0, left)
            right = jnp.where(lane == lanes - 1, 0.0, right)
    return (below + above + (down + up)) + along * (left + right)


def chunk_of(planes, most):
    best = planes
    for number in range(2, most + 1, 2):
        if planes % number == 0:
            best = number
    return best if planes > most else planes


def for_planes(planes, most, body):
    chunk = chunk_of(planes, most)
    if chunk == planes:
        body(0, planes)
        return

    def step(number, carry):
        body(number * chunk, chunk)
        return carry

    lax.fori_loop(0, planes // chunk, step, 0)


def half(field, source, masks, colour, keep, size, shape, most):
    planes, rows, lanes = shape

    def body(start, count):
        old = [field[start + number] for number in range(count + 2)]
        for number in range(count):
            here = old[number + 1]
            total = beside_sum(old[number], here, old[number + 2], size, rows, lanes)
            update = (source[start + number] + total) * inverse
            chosen = masks((number + colour) % 2, keep(start + number))
            field[start + number + 1] = jnp.where(chosen, update, here)

    for_planes(planes, most, body)


def first_half(field, source, masks, keep, shape, most):
    planes, rows, lanes = shape
    field[0] = jnp.zeros((rows, lanes), F32)
    field[planes + 1] = jnp.zeros((rows, lanes), F32)

    def body(start, count):
        for number in range(count):
            chosen = masks(number % 2, keep(start + number))
            field[start + number + 1] = jnp.where(chosen, source[start + number] * inverse, 0.0)

    for_planes(planes, most, body)


def sweeps(field, source, masks, keep, size, shape, most, halves):
    for colour in halves:
        half(field, source, masks, colour, keep, size, shape, most)


def restricted(field, source, pairs, first, block, size, shape, most):
    planes, rows, lanes = shape
    height = pairs.shape[1]
    count_x, count_y, count_z = block
    top = min(height, up_to(count_y, 8))
    if height > top:
        pairs[0 : count_x // 2, top:height] = jnp.zeros((count_x // 2, height - top, LANES), F32)

    def body(start, count):
        old = [field[first + start + number] for number in range(count + 2)]
        parts = []
        for number in range(count):
            here = old[number + 1]
            total = beside_sum(old[number], here, old[number + 2], size, rows, lanes)
            rest = source[first + start + number] - centre * here + total
            parts.append(rest[:top, :LANES])
        half_start = start // 2 if isinstance(start, int) else lax.div(start, 2)
        for number in range(count // 2):
            both = parts[2 * number] + parts[2 * number + 1]
            if top > count_y:
                both = jnp.where(iota(both.shape, 0) < count_y, both, 0.0)
            pairs[half_start + number, 0:top] = both

    for_planes(count_x, most, body)
    number = count_x // 2
    even = pairs[0:number, pl.ds(0, height // 2, stride=2), :]
    odd = pairs[0:number, pl.ds(1, height // 2, stride=2), :]
    lane, column = iota((LANES, LANES), 0), iota((LANES, LANES), 1)
    down = jnp.where((lane // 2 == column) & (lane < count_z), 0.5, 0.0).astype(F32)
    flat = (even + odd).reshape(number * (height // 2), LANES)
    return dot(flat, down).reshape(number, height // 2, LANES)


def device(place, steps):
    return tuple(place[which] + steps[which] for which in range(3))


def exists(place, steps, counts):
    found = None
    for which in range(3):
        if steps[which] == 0:
            continue
        other = place[which] + steps[which]
        here = (other >= 0) & (other < counts[which])
        found = here if found is None else found & here
    return found


class Exchange:
    def __init__(self, level, place, array, offset, refs):
        self.level, self.place, self.array, self.offset = level, place, array, offset
        (self.stage_x, self.land_x, self.land_y, self.stage_y) = refs[:4]
        (self.stage_z, self.land_z, self.sent, self.got) = refs[4:]

    def xy(self, number):
        level = self.level
        dx, dy = STEPS_XY[number]
        margin, length = level.margins[0], level.block[0]
        place = {1: 0, 0: margin, -1: margin + length}[dx]
        count = length if dx == 0 else margin
        origin = length - margin if dx == 1 else 0
        if dy == 0:
            source = self.stage_x.at[(dx + 1) // 2]
            target = self.land_x.at[(dx + 1) // 2]
        else:
            source = self.stage_y.at[(dy + 1) // 2, pl.ds(origin, count)]
            target = self.land_y.at[(dy + 1) // 2, pl.ds(place, count)]
        return (dx, dy, 0), (place, count), pltpu.make_async_remote_copy(
            src_ref=source,
            dst_ref=target,
            send_sem=self.sent.at[number],
            recv_sem=self.got.at[number],
            device_id=device(self.place, (dx, dy, 0)),
            device_id_type=pl.DeviceIdType.MESH,
        )

    def start_xy(self):
        level, array = self.level, self.array
        low = self.offset + level.margins[0]
        length, rows, margin = level.block[0], level.block[1], level.margins
        self.stage_y[0] = array[low : low + length, 0 : margin[1], 0:LANES]
        self.stage_y[1] = array[low : low + length, rows - margin[1] : rows, 0:LANES]
        self.stage_x[0] = array[low : low + margin[0], 0:rows, 0:LANES]
        self.stage_x[1] = array[low + length - margin[0] : low + length, 0:rows, 0:LANES]
        for number in range(8):
            steps, _, copy = self.xy(number)

            @pl.when(exists(self.place, steps, level.counts))
            def _():
                copy.start()

    def finish_xy(self):
        level, array = self.level, self.array
        rows, margin = level.block[1], level.margins[1]
        for number in range(8):
            steps, (place, count), copy = self.xy(number)
            back = tuple(-step for step in steps)

            @pl.when(exists(self.place, back, level.counts))
            def _():
                copy.wait_recv()
                low = self.offset + place
                if steps[1] == 0:
                    array[low : low + count, 0:rows, 0:LANES] = self.land_x[(steps[0] + 1) // 2]
                else:
                    first = level.rows - margin if steps[1] == 1 else rows
                    side = (steps[1] + 1) // 2
                    array[low : low + count, first : first + margin, 0:LANES] = self.land_y[
                        side, place : place + count
                    ]

    def z(self, side):
        return pltpu.make_async_remote_copy(
            src_ref=self.stage_z.at[side],
            dst_ref=self.land_z.at[side],
            send_sem=self.sent.at[8 + side],
            recv_sem=self.got.at[8 + side],
            device_id=device(self.place, (0, 0, 2 * side - 1)),
            device_id_type=pl.DeviceIdType.MESH,
        )

    def start_z(self):
        level, array = self.level, self.array
        margin, length = level.margins[2], level.block[2]
        lane = iota((level.rows, LANES), 1)
        for side in range(2):
            first = length - margin if side == 1 else 0
            for pack in range(level.packs):
                total = jnp.zeros((level.rows, LANES), F32)
                for number in range(min(level.per, level.planes - pack * level.per)):
                    plane = array[self.offset + pack * level.per + number, :, 0:LANES]
                    moved = pltpu.roll(plane, (number * margin - first) % LANES, 1)
                    total = jnp.where(lane // margin == number, moved, total)
                self.stage_z[side, pack] = total
        for side in range(2):
            @pl.when(exists(self.place, (0, 0, 2 * side - 1), level.counts))
            def _():
                self.z(side).start()

    def finish_z(self):
        level, array = self.level, self.array
        margin, length = level.margins[2], level.block[2]
        base = level.lanes - LANES
        lane = iota((level.rows, LANES), 1)
        have = []
        for side in range(2):
            there = exists(self.place, (0, 0, 1 - 2 * side), level.counts)
            have.append(there)

            @pl.when(there)
            def _():
                self.z(side).wait_recv()

        above = length - base
        take_above = (lane >= above) & (lane < above + margin) & have[0]
        take_below = (lane >= LANES - margin) & have[1]
        for pack in range(level.packs):
            from_above, from_below = self.land_z[0, pack], self.land_z[1, pack]
            for number in range(min(level.per, level.planes - pack * level.per)):
                plane = self.offset + pack * level.per + number
                high = pltpu.roll(from_above, (above - number * margin) % LANES, 1)
                low = pltpu.roll(from_below, (LANES - margin - number * margin) % LANES, 1)
                value = array[plane, :, base : level.lanes]
                value = jnp.where(take_above, high, value)
                array[plane, :, base : level.lanes] = jnp.where(take_below, low, value)

    def drain(self):
        for number in range(8):
            steps, _, copy = self.xy(number)

            @pl.when(exists(self.place, steps, self.level.counts))
            def _():
                copy.wait_send()

        for side in range(2):
            @pl.when(exists(self.place, (0, 0, 2 * side - 1), self.level.counts))
            def _():
                self.z(side).wait_send()


def solve_whole(levels, refs, pairs, number):
    level = levels[number]
    source, field = refs[number]
    planes, rows, lanes = level.shape
    row, lane = iota((rows, lanes), 0), iota((rows, lanes), 1)
    inside = (row < level.size[1]) & (lane < level.size[2])
    choices = [inside & ((row + lane) % 2 == colour) for colour in range(2)]

    def masks(which, keep):
        return choices[which]

    def keep(plane):
        return None

    first_half(field, source, masks, keep, level.shape, 8)
    if number == len(levels) - 1:
        sweeps(field, source, masks, keep, level.size, level.shape, 8, (1,) + (0, 1) * (CSWEEPS - 1))
        return
    sweeps(field, source, masks, keep, level.size, level.shape, 8, (1, 0, 1))
    coarse = levels[number + 1]
    height = 2 * coarse.rows
    hold = pairs.at[:, 0:height]
    below = restricted(field, source, hold, 0, level.size, level.size, level.shape, 8)
    refs[number + 1][0][...] = below
    solve_whole(levels, refs, pairs, number + 1)
    count = coarse.shape[0]
    solved = refs[number + 1][1][1 : 1 + count]
    column, target = iota((LANES, LANES), 0), iota((LANES, LANES), 1)
    spread = jnp.where(target // 2 == column, 1.0, 0.0).astype(F32)
    flat = dot(solved.reshape(count * coarse.rows, LANES), spread)
    flat = flat.reshape(count, coarse.rows, LANES)
    pairs[0:count, pl.ds(0, coarse.rows, stride=2), :] = flat
    pairs[0:count, pl.ds(1, coarse.rows, stride=2), :] = flat
    for plane in range(planes):
        field[plane + 1] = field[plane + 1] + pairs[plane // 2, 0:rows]
    sweeps(field, source, masks, keep, level.size, level.shape, 8, (0, 1, 0, 1))


def kernel(splits, levels, counts, density, potential, *refs):
    place = tuple(lax.axis_index(axis) for axis in AXES)
    total = counts[0] * counts[1] * counts[2]
    me = (place[0] * counts[1] + place[1]) * counts[2] + place[2]
    refs = list(refs)

    def take(number):
        taken = refs[:number]
        del refs[:number]
        return taken

    parts = []
    for level in splits:
        source, field, mask = take(3)
        of_source = Exchange(level, place, source, 0, take(8))
        of_field = Exchange(level, place, field, 1, take(8))
        parts.append((source, field, mask, of_source, of_field))
    whole_refs = [take(2) for _ in levels]
    pairs, spreads, own, slots, sent, got = take(6)

    def peer(number):
        other = lax.rem(me + number, total)
        inner = counts[1] * counts[2]
        return (lax.div(other, inner), lax.rem(lax.div(other, counts[2]), counts[1]), lax.rem(other, counts[2])), other

    barrier = pltpu.get_barrier_semaphore()

    def greet(number, carry):
        pl.semaphore_signal(
            barrier, inc=1, device_id=peer(number)[0], device_id_type=pl.DeviceIdType.MESH
        )
        return carry

    lax.fori_loop(1, total, greet, 0)

    for level, (source, field, mask, of_source, of_field) in zip(splits, parts):
        source[...] = jnp.zeros(level.shape, F32)
        plane = (level.rows, level.lanes)
        inside = None
        for dim in (1, 2):
            index = iota(plane, dim - 1)
            size = level.rows if dim == 1 else level.lanes
            margin, length = level.margins[dim], level.block[dim]
            used = (index < length + margin) | (index >= size - margin)
            spot = local_of(index, length, margin, size) + place[dim] * length
            used = used & (spot >= 0) & (spot < length * counts[dim])
            inside = used if inside is None else inside & used
        parity = (iota(plane, 0) + iota(plane, 1)) % 2
        for colour in range(2):
            mask[colour] = jnp.where(inside & (parity == colour), 1, 0)
    first = splits[0]
    parts[0][0][
        first.margins[0] : first.margins[0] + first.block[0], 0 : first.block[1], 0 : first.block[2]
    ] = density[...]
    pl.semaphore_wait(barrier, total - 1)

    def keep_of(level):
        def keep(plane):
            spot = place[0] * level.block[0] + plane - level.margins[0]
            return jnp.where((spot >= 0) & (spot < level.block[0] * counts[0]), 1, 0)

        return keep

    def masks_of(mask):
        def masks(which, keep):
            return (mask[which] & keep) != 0

        return masks

    def descend(number):
        level = splits[number]
        source, field, mask, of_source, _ = parts[number]
        masks, keep = masks_of(mask), keep_of(level)
        first_half(field, source, masks, keep, level.shape, 8)
        sweeps(field, source, masks, keep, None, level.shape, 8, (1, 0, 1))
        height = 2 * up_to(level.block[1] // 2, 8)
        return restricted(
            field, source, pairs.at[:, 0:height], level.margins[0], level.block, None, level.shape, 8
        )

    def ascend(number, coarse_plane, rows_to, lanes_to, reach):
        level = splits[number]
        source, field, mask, _, _ = parts[number]
        masks, keep = masks_of(mask), keep_of(level)
        for spot in range(reach):
            spreads[spot] = dot(rows_to, coarse_plane(spot))
        flat = dot(spreads[0:reach].reshape(reach * level.rows, LANES), lanes_to)
        flat = flat.reshape(reach, level.rows, level.lanes)
        for plane in range(level.planes):
            added = jnp.where(keep(plane) != 0, flat[plane // 2], 0.0)
            field[plane + 1] = field[plane + 1] + added
        sweeps(field, source, masks, keep, None, level.shape, 8, (0, 1, 0, 1))

    top, next_ = splits
    top_parts, next_parts = parts
    top_parts[3].start_xy()
    top_parts[3].finish_xy()
    top_parts[3].start_z()
    top_parts[3].finish_z()
    below = descend(0)
    next_parts[0][
        next_.margins[0] : next_.margins[0] + next_.block[0], 0 : next_.block[1], 0:LANES
    ] = below
    next_parts[3].start_xy()
    top_parts[4].start_xy()
    next_parts[3].finish_xy()
    next_parts[3].start_z()
    next_parts[3].finish_z()
    below = descend(1)

    length = tuple(size // 2 for size in next_.block)
    per = LANES // length[2]
    packed = jnp.zeros((8, LANES), F32)
    for plane in range(length[0]):
        moved = below[plane]
        if plane // per:
            moved = pltpu.roll(moved, length[1] * (plane // per), 0)
        if plane % per:
            moved = pltpu.roll(moved, length[2] * (plane % per), 1)
        packed = packed + moved
    own[...] = packed
    slots[me] = packed

    def send(number):
        target, other = peer(number)
        return pltpu.make_async_remote_copy(
            src_ref=own,
            dst_ref=slots.at[me],
            send_sem=sent.at[other],
            recv_sem=got.at[me],
            device_id=target,
            device_id_type=pl.DeviceIdType.MESH,
        )

    def start_send(number, carry):
        send(number).start()
        return carry

    lax.fori_loop(1, total, start_send, 0)
    next_parts[4].start_xy()
    top_parts[4].finish_xy()
    top_parts[4].start_z()
    next_parts[4].finish_xy()
    next_parts[4].start_z()

    def finish_send(number, carry):
        target, other = peer(number)
        copy = pltpu.make_async_remote_copy(
            src_ref=own,
            dst_ref=slots.at[other],
            send_sem=sent.at[other],
            recv_sem=got.at[other],
            device_id=target,
            device_id_type=pl.DeviceIdType.MESH,
        )
        copy.wait_recv()
        copy.wait_send()
        return carry

    lax.fori_loop(1, total, finish_send, 0)

    coarse_source, coarse_field = whole_refs[0]
    lane = iota((8, LANES), 1)

    def place_x(which, carry):
        for second in range(counts[1]):
            base = (which * counts[1] + second) * counts[2]
            tiles = [slots[base + third] for third in range(counts[2])]
            for spot in range(per):
                value = jnp.zeros((8, LANES), F32)
                for third in range(counts[2]):
                    shift = (length[2] * (third - spot)) % LANES
                    moved = pltpu.roll(tiles[third], shift, 1) if shift else tiles[third]
                    value = jnp.where(lane // length[2] == third, moved, value)
                for group in range(8 // length[1]):
                    plane = which * length[0] + group * per + spot
                    coarse_source[plane, second * length[1] : (second + 1) * length[1], :] = value[
                        group * length[1] : (group + 1) * length[1]
                    ]
        return carry

    lax.fori_loop(0, counts[0], place_x, 0)
    solve_whole(levels, whole_refs, pairs, 0)

    def one_hot(shape, dim, fine, fine_length, fine_margin, origin, wrap):
        index = iota(shape, dim)
        spot = local_of(index, fine_length, fine_margin, fine)
        cell = jnp.where(spot >= 0, lax.div(spot, 2), -lax.div(1 - spot, 2)) + origin
        if wrap is not None:
            cell = jnp.where(cell < 0, cell + wrap, cell)
        used = (index < fine_length + fine_margin) | (index >= fine - fine_margin)
        return jnp.where((iota(shape, 1 - dim) == cell) & used, 1.0, 0.0).astype(F32)

    coarse = levels[0]
    rows_to = one_hot(
        (next_.rows, coarse.rows), 0, next_.rows, next_.block[1], next_.margins[1],
        place[1] * length[1], None,
    )
    lanes_to = one_hot(
        (LANES, next_.lanes), 1, next_.lanes, next_.block[2], next_.margins[2],
        place[2] * length[2], None,
    )
    reach = next_.planes // 2

    def plane_of_whole(spot):
        plane = place[0] * length[0] + spot - next_.margins[0] // 2
        return coarse_field[1 + jnp.clip(plane, 0, coarse.shape[0] - 1)]

    next_parts[4].finish_z()
    ascend(1, plane_of_whole, rows_to, lanes_to, reach)

    rows_to = one_hot(
        (top.rows, next_.rows), 0, top.rows, top.block[1], top.margins[1], 0, next_.rows
    )
    lanes_to = one_hot(
        (LANES, top.lanes), 1, top.lanes, top.block[2], top.margins[2], 0, next_.lanes
    )
    shift = next_.margins[0] - top.margins[0] // 2
    top_parts[4].finish_z()
    ascend(0, lambda spot: next_parts[1][1 + spot + shift], rows_to, lanes_to, top.planes // 2)
    potential[...] = top_parts[1][
        1 + top.margins[0] : 1 + top.margins[0] + top.block[0], 0 : top.block[1], 0 : top.block[2]
    ]
    for part in parts:
        part[3].drain()
        part[4].drain()


def flat_scratch(entries):
    out = []
    for entry in entries:
        out.extend(flat_scratch(entry) if isinstance(entry, (list, tuple)) else [entry])
    return out


def on_device(counts, density):
    block = density.shape
    half_block = tuple(size // 2 for size in block)
    splits = [
        Split(block, (4, 4, 4), counts),
        Split(half_block, (6, 8, 8), counts),
    ]
    size = tuple(block[which] * counts[which] // 4 for which in range(3))
    levels = []
    for number in range(2, LEVELS):
        levels.append(Whole(size))
        size = tuple(max(part // 2, 1) for part in size)
    total = counts[0] * counts[1] * counts[2]
    pair_planes = max(block[0] // 2, levels[0].shape[0])
    pair_rows = max(block[1], levels[0].rows, 16)
    scratch = [level.scratch() for level in splits] + [level.scratch() for level in levels]
    scratch = flat_scratch(scratch) + [
        pltpu.VMEM((pair_planes, pair_rows, LANES), F32),
        pltpu.VMEM((max(level.planes // 2 for level in splits), splits[0].rows, LANES), F32),
        pltpu.VMEM((8, LANES), F32),
        pltpu.VMEM((total, 8, LANES), F32),
        pltpu.SemaphoreType.DMA((total,)),
        pltpu.SemaphoreType.DMA((total,)),
    ]
    return pl.pallas_call(
        functools.partial(kernel, splits, levels, counts),
        out_shape=jax.ShapeDtypeStruct(block, F32),
        in_specs=[pl.BlockSpec(memory_space=pltpu.VMEM)],
        out_specs=pl.BlockSpec(memory_space=pltpu.VMEM),
        scratch_shapes=scratch,
        compiler_params=pltpu.CompilerParams(
            collective_id=0, has_side_effects=True, vmem_limit_bytes=48 * 1024 * 1024
        ),
    )(density)


def solution(mesh):
    counts = tuple(mesh.shape[axis] for axis in AXES)
    return jax.shard_map(
        functools.partial(on_device, counts),
        mesh=mesh,
        in_specs=(P("gx", "gy", "gz"),),
        out_specs=P("gx", "gy", "gz"),
        check_vma=False,
    )
```

```python
import functools

import jax
import jax.numpy as jnp
from jax import lax
from jax.experimental import pallas as pl
from jax.experimental.pallas import tpu as pltpu
from jax.sharding import PartitionSpec as P

LEVELS = 7
CSWEEPS = 4
rsd_beta = 0.5
centre = 4.0 + 2.0 * (1.0 + rsd_beta)
along = 1.0 + rsd_beta
inverse = 1.0 / centre
F32 = jnp.float32
LANES = 128
AXES = ("gx", "gy", "gz")
STEPS_XY = [(dx, dy) for dx in (-1, 0, 1) for dy in (-1, 0, 1) if (dx, dy) != (0, 0)]


def up_to(value, unit):
    return -(-value // unit) * unit


class Split:
    def __init__(self, block, margins, counts):
        self.block, self.margins, self.counts = block, margins, counts
        self.planes = block[0] + 2 * margins[0]
        self.rows = up_to(block[1] + 2 * margins[1], 8)
        self.lanes = up_to(block[2] + 2 * margins[2], LANES)
        self.per = LANES // margins[2]
        self.packs = -(-self.planes // self.per)
        self.shape = (self.planes, self.rows, self.lanes)

    def scratch(self):
        land_x = (2, self.margins[0], self.block[1], LANES)
        land_y = (2, self.planes, self.margins[1], LANES)
        stage_y = (2, self.block[0], self.margins[1], LANES)
        packed = (2, self.packs, self.rows, LANES)
        one = [
            pltpu.VMEM(land_x, F32),
            pltpu.VMEM(land_x, F32),
            pltpu.VMEM(land_y, F32),
            pltpu.VMEM(stage_y, F32),
            pltpu.VMEM(packed, F32),
            pltpu.VMEM(packed, F32),
            pltpu.SemaphoreType.DMA((10,)),
            pltpu.SemaphoreType.DMA((10,)),
        ]
        own = [
            pltpu.VMEM(self.shape, F32),
            pltpu.VMEM((self.planes + 2,) + self.shape[1:], F32),
            pltpu.VMEM((2,) + self.shape[1:], jnp.int32),
        ]
        return own, one, list(one)


class Whole:
    def __init__(self, size):
        self.size = size
        self.rows = up_to(size[1], 8)
        self.lanes = up_to(size[2], LANES)
        self.shape = (size[0], self.rows, self.lanes)

    def scratch(self):
        return [
            pltpu.VMEM(self.shape, F32),
            pltpu.VMEM((self.shape[0] + 2,) + self.shape[1:], F32),
        ]


def iota(shape, dim):
    return lax.broadcasted_iota(jnp.int32, shape, dim)


def pieces(value):
    high = value.astype(jnp.bfloat16)
    rest = value - high.astype(F32)
    middle = rest.astype(jnp.bfloat16)
    return high, middle, (rest - middle.astype(F32)).astype(jnp.bfloat16)


def dot(value, chosen):
    chosen = chosen.astype(jnp.bfloat16)
    parts = [jnp.dot(part, chosen, preferred_element_type=F32) for part in pieces(value)]
    return parts[0] + (parts[1] + parts[2])


def dot_rows(chosen, value):
    return jnp.dot(chosen, value, precision=lax.Precision.HIGHEST, preferred_element_type=F32)


def local_of(index, length, margin, total):
    return jnp.where(index < total - margin, index, index - total)


def beside_sum(below, here, above, size, rows, lanes):
    down, up = pltpu.roll(here, 1, 0), pltpu.roll(here, rows - 1, 0)
    left, right = pltpu.roll(here, 1, 1), pltpu.roll(here, lanes - 1, 1)
    if size is not None:
        if size[1] == rows:
            row = iota(here.shape, 0)
            down = jnp.where(row == 0, 0.0, down)
            up = jnp.where(row == rows - 1, 0.0, up)
        if size[2] == lanes:
            lane = iota(here.shape, 1)
            left = jnp.where(lane == 0, 0.0, left)
            right = jnp.where(lane == lanes - 1, 0.0, right)
    return (below + above + (down + up)) + along * (left + right)


def chunk_of(planes, most):
    if planes <= most:
        return planes
    return max([number for number in range(2, most + 1, 2) if planes % number == 0])


def for_planes(first, planes, most, body):
    chunk = chunk_of(planes, most)
    if chunk == planes:
        body(first, planes)
        return

    def step(number, carry):
        body(first + number * chunk, chunk)
        return carry

    lax.fori_loop(0, planes // chunk, step, 0)


def half(field, source, masks, colour, keep, size, shape, most, skip=0):
    planes, rows, lanes = shape

    def body(start, count):
        before, here = field[start], field[start + 1]
        for number in range(count):
            after = field[start + number + 2]
            total = beside_sum(before, here, after, size, rows, lanes)
            update = (source[start + number] + total) * inverse
            chosen = masks((number + skip + colour) % 2, keep(start + number))
            field[start + number + 1] = jnp.where(chosen, update, here)
            before, here = here, after

    for_planes(skip, planes - 2 * skip, most, body)


def first_half(field, source, masks, keep, shape, most):
    planes, rows, lanes = shape
    field[0] = jnp.zeros((rows, lanes), F32)
    field[planes + 1] = jnp.zeros((rows, lanes), F32)

    def body(start, count):
        for number in range(count):
            chosen = masks(number % 2, keep(start + number))
            field[start + number + 1] = jnp.where(chosen, source[start + number] * inverse, 0.0)

    for_planes(0, planes, most, body)


def sweeps(field, source, masks, keep, size, shape, most, halves, skips=None):
    for number, colour in enumerate(halves):
        skip = 0 if skips is None else skips[number]
        half(field, source, masks, colour, keep, size, shape, most, skip)


def restricted(field, source, pairs, first, block, size, shape, most):
    planes, rows, lanes = shape
    height = pairs.shape[1]
    count_x, count_y, count_z = block
    top = min(height, up_to(count_y, 8))
    if height > top:
        pairs[0 : count_x // 2, top:height] = jnp.zeros((count_x // 2, height - top, LANES), F32)

    def body(start, count):
        old = [field[first + start + number] for number in range(count + 2)]
        parts = []
        for number in range(count):
            here = old[number + 1]
            total = beside_sum(old[number], here, old[number + 2], size, rows, lanes)
            rest = source[first + start + number] - centre * here + total
            parts.append(rest[:top, :LANES])
        half_start = start // 2 if isinstance(start, int) else lax.div(start, 2)
        for number in range(count // 2):
            both = parts[2 * number] + parts[2 * number + 1]
            if top > count_y:
                both = jnp.where(iota(both.shape, 0) < count_y, both, 0.0)
            pairs[half_start + number, 0:top] = both

    for_planes(0, count_x, most, body)
    number = count_x // 2
    even = pairs[0:number, pl.ds(0, height // 2, stride=2), :]
    odd = pairs[0:number, pl.ds(1, height // 2, stride=2), :]
    lane, column = iota((LANES, LANES), 0), iota((LANES, LANES), 1)
    down = jnp.where((lane // 2 == column) & (lane < count_z), 0.5, 0.0).astype(F32)
    flat = (even + odd).reshape(number * (height // 2), LANES)
    return dot(flat, down).reshape(number, height // 2, LANES)


def device(place, steps):
    return tuple(place[which] + steps[which] for which in range(3))


def exists(place, steps, counts):
    found = None
    for which in range(3):
        if steps[which] == 0:
            continue
        other = place[which] + steps[which]
        here = (other >= 0) & (other < counts[which])
        found = here if found is None else found & here
    return found


class Exchange:
    def __init__(self, level, place, array, offset, refs):
        self.level, self.place, self.array, self.offset = level, place, array, offset
        (self.stage_x, self.land_x, self.land_y, self.stage_y) = refs[:4]
        (self.stage_z, self.land_z, self.sent, self.got) = refs[4:]

    def xy(self, number):
        level = self.level
        dx, dy = STEPS_XY[number]
        margin, length = level.margins[0], level.block[0]
        place = {1: 0, 0: margin, -1: margin + length}[dx]
        count = length if dx == 0 else margin
        origin = length - margin if dx == 1 else 0
        if dy == 0:
            source = self.stage_x.at[(dx + 1) // 2]
            target = self.land_x.at[(dx + 1) // 2]
        else:
            source = self.stage_y.at[(dy + 1) // 2, pl.ds(origin, count)]
            target = self.land_y.at[(dy + 1) // 2, pl.ds(place, count)]
        return (dx, dy, 0), (place, count), pltpu.make_async_remote_copy(
            src_ref=source,
            dst_ref=target,
            send_sem=self.sent.at[number],
            recv_sem=self.got.at[number],
            device_id=device(self.place, (dx, dy, 0)),
            device_id_type=pl.DeviceIdType.MESH,
        )

    def start_xy(self):
        level, array = self.level, self.array
        low = self.offset + level.margins[0]
        length, rows, margin = level.block[0], level.block[1], level.margins
        self.stage_y[0] = array[low : low + length, 0 : margin[1], 0:LANES]
        self.stage_y[1] = array[low : low + length, rows - margin[1] : rows, 0:LANES]
        self.stage_x[0] = array[low : low + margin[0], 0:rows, 0:LANES]
        self.stage_x[1] = array[low + length - margin[0] : low + length, 0:rows, 0:LANES]
        for number in range(8):
            steps, _, copy = self.xy(number)

            @pl.when(exists(self.place, steps, level.counts))
            def _():
                copy.start()

    def finish_xy(self):
        level, array = self.level, self.array
        rows, margin = level.block[1], level.margins[1]
        for number in range(8):
            steps, (place, count), copy = self.xy(number)
            back = tuple(-step for step in steps)

            @pl.when(exists(self.place, back, level.counts))
            def _():
                copy.wait_recv()
                low = self.offset + place
                if steps[1] == 0:
                    array[low : low + count, 0:rows, 0:LANES] = self.land_x[(steps[0] + 1) // 2]
                else:
                    first = level.rows - margin if steps[1] == 1 else rows
                    side = (steps[1] + 1) // 2
                    array[low : low + count, first : first + margin, 0:LANES] = self.land_y[
                        side, place : place + count
                    ]

    def z(self, side):
        return pltpu.make_async_remote_copy(
            src_ref=self.stage_z.at[side],
            dst_ref=self.land_z.at[side],
            send_sem=self.sent.at[8 + side],
            recv_sem=self.got.at[8 + side],
            device_id=device(self.place, (0, 0, 2 * side - 1)),
            device_id_type=pl.DeviceIdType.MESH,
        )

    def start_z(self):
        level, array = self.level, self.array
        margin, length = level.margins[2], level.block[2]
        lane = iota((level.rows, LANES), 1)
        for side in range(2):
            first = length - margin if side == 1 else 0
            for pack in range(level.packs):
                total = jnp.zeros((level.rows, LANES), F32)
                for number in range(min(level.per, level.planes - pack * level.per)):
                    plane = array[self.offset + pack * level.per + number, :, 0:LANES]
                    moved = pltpu.roll(plane, (number * margin - first) % LANES, 1)
                    total = jnp.where(lane // margin == number, moved, total)
                self.stage_z[side, pack] = total
        for side in range(2):
            @pl.when(exists(self.place, (0, 0, 2 * side - 1), level.counts))
            def _():
                self.z(side).start()

    def finish_z(self):
        level, array = self.level, self.array
        margin, length = level.margins[2], level.block[2]
        base = level.lanes - LANES
        lane = iota((level.rows, LANES), 1)
        have = []
        for side in range(2):
            there = exists(self.place, (0, 0, 1 - 2 * side), level.counts)
            have.append(there)

            @pl.when(there)
            def _():
                self.z(side).wait_recv()

        above = length - base
        take_above = (lane >= above) & (lane < above + margin) & have[0]
        take_below = (lane >= LANES - margin) & have[1]
        for pack in range(level.packs):
            from_above, from_below = self.land_z[0, pack], self.land_z[1, pack]
            for number in range(min(level.per, level.planes - pack * level.per)):
                plane = self.offset + pack * level.per + number
                high = pltpu.roll(from_above, (above - number * margin) % LANES, 1)
                low = pltpu.roll(from_below, (LANES - margin - number * margin) % LANES, 1)
                value = array[plane, :, base : level.lanes]
                value = jnp.where(take_above, high, value)
                array[plane, :, base : level.lanes] = jnp.where(take_below, low, value)

    def drain(self):
        for number in range(8):
            steps, _, copy = self.xy(number)

            @pl.when(exists(self.place, steps, self.level.counts))
            def _():
                copy.wait_send()

        for side in range(2):
            @pl.when(exists(self.place, (0, 0, 2 * side - 1), self.level.counts))
            def _():
                self.z(side).wait_send()


def solve_whole(levels, refs, pairs, number):
    level = levels[number]
    source, field = refs[number]
    planes, rows, lanes = level.shape
    row, lane = iota((rows, lanes), 0), iota((rows, lanes), 1)
    inside = (row < level.size[1]) & (lane < level.size[2])
    choices = [inside & ((row + lane) % 2 == colour) for colour in range(2)]

    def masks(which, keep):
        return choices[which]

    def keep(plane):
        return None

    first_half(field, source, masks, keep, level.shape, 16)
    if number == len(levels) - 1:
        sweeps(field, source, masks, keep, level.size, level.shape, 16, (1,) + (0, 1) * (CSWEEPS - 1))
        return
    sweeps(field, source, masks, keep, level.size, level.shape, 16, (1, 0, 1))
    coarse = levels[number + 1]
    height = 2 * coarse.rows
    hold = pairs.at[:, 0:height]
    below = restricted(field, source, hold, 0, level.size, level.size, level.shape, 16)
    refs[number + 1][0][...] = below
    solve_whole(levels, refs, pairs, number + 1)
    count = coarse.shape[0]
    solved = refs[number + 1][1][1 : 1 + count]
    column, target = iota((LANES, LANES), 0), iota((LANES, LANES), 1)
    spread = jnp.where(target // 2 == column, 1.0, 0.0).astype(F32)
    flat = dot(solved.reshape(count * coarse.rows, LANES), spread)
    flat = flat.reshape(count, coarse.rows, LANES)
    pairs[0:count, pl.ds(0, coarse.rows, stride=2), :] = flat
    pairs[0:count, pl.ds(1, coarse.rows, stride=2), :] = flat
    for plane in range(planes):
        field[plane + 1] = field[plane + 1] + pairs[plane // 2, 0:rows]
    sweeps(field, source, masks, keep, level.size, level.shape, 16, (0, 1, 0, 1))


def kernel(splits, levels, counts, density, potential, *refs):
    place = tuple(lax.axis_index(axis) for axis in AXES)
    total = counts[0] * counts[1] * counts[2]
    me = (place[0] * counts[1] + place[1]) * counts[2] + place[2]
    refs = list(refs)

    def take(number):
        taken = refs[:number]
        del refs[:number]
        return taken

    parts = []
    for level in splits:
        source, field, mask = take(3)
        of_source = Exchange(level, place, source, 0, take(8))
        of_field = Exchange(level, place, field, 1, take(8))
        parts.append((source, field, mask, of_source, of_field))
    whole_refs = [take(2) for _ in levels]
    pairs, spreads, own, slots, sent, got = take(6)

    def peer(number):
        other = lax.rem(me + number, total)
        inner = counts[1] * counts[2]
        return (lax.div(other, inner), lax.rem(lax.div(other, counts[2]), counts[1]), lax.rem(other, counts[2])), other

    barrier = pltpu.get_barrier_semaphore()

    def greet(number, carry):
        pl.semaphore_signal(
            barrier, inc=1, device_id=peer(number)[0], device_id_type=pl.DeviceIdType.MESH
        )
        return carry

    lax.fori_loop(1, total, greet, 0)

    first = splits[0]
    parts[0][0][
        first.margins[0] : first.margins[0] + first.block[0], 0 : first.block[1], 0 : first.block[2]
    ] = density[...]
    pl.semaphore_wait(barrier, total - 1)

    parts[0][3].start_xy()

    for level, (source, field, mask, of_source, of_field) in zip(splits, parts):
        plane = (level.rows, level.lanes)
        inside = None
        for dim in (1, 2):
            index = iota(plane, dim - 1)
            size = level.rows if dim == 1 else level.lanes
            margin, length = level.margins[dim], level.block[dim]
            used = (index < length + margin) | (index >= size - margin)
            spot = local_of(index, length, margin, size) + place[dim] * length
            used = used & (spot >= 0) & (spot < length * counts[dim])
            inside = used if inside is None else inside & used
        parity = (iota(plane, 0) + iota(plane, 1)) % 2
        for colour in range(2):
            mask[colour] = jnp.where(inside & (parity == colour), 1, 0)

    def keep_of(level):
        def keep(plane):
            spot = place[0] * level.block[0] + plane - level.margins[0]
            return jnp.where((spot >= 0) & (spot < level.block[0] * counts[0]), 1, 0)

        return keep

    def masks_of(mask):
        def masks(which, keep):
            return (mask[which] & keep) != 0

        return masks

    edges = [level.margins[0] for level in splits]
    before = [tuple(edge - reach for reach in (3, 2, 1)) for edge in edges]
    final = (0, splits[0].margins[0] // 2)
    after = [
        tuple(edge - reach - last for reach in (3, 2, 1, 0)) for edge, last in zip(edges, final)
    ]
    before[0] = tuple(skip - skip % 2 for skip in before[0])
    after[0] = tuple(skip - skip % 2 for skip in after[0])

    def descend(number):
        level = splits[number]
        source, field, mask, of_source, _ = parts[number]
        masks, keep = masks_of(mask), keep_of(level)
        first_half(field, source, masks, keep, level.shape, 20)
        sweeps(field, source, masks, keep, None, level.shape, 26, (1, 0, 1), before[number])
        height = 2 * up_to(level.block[1] // 2, 8)
        return restricted(
            field, source, pairs.at[:, 0:height], level.margins[0], level.block, None, level.shape, 16
        )

    def ascend(number, coarse_plane, rows_to, lanes_to, reach):
        level = splits[number]
        source, field, mask, _, _ = parts[number]
        masks, keep = masks_of(mask), keep_of(level)
        for spot in range(reach):
            spreads[spot] = dot_rows(rows_to, coarse_plane(spot))
        flat = dot(spreads[0:reach].reshape(reach * level.rows, LANES), lanes_to)
        flat = flat.reshape(reach, level.rows, level.lanes)
        for plane in range(level.planes):
            added = jnp.where(keep(plane) != 0, flat[plane // 2], 0.0)
            field[plane + 1] = field[plane + 1] + added
        sweeps(field, source, masks, keep, None, level.shape, 26, (0, 1, 0, 1), after[number])

    top, next_ = splits
    top_parts, next_parts = parts
    top_parts[3].finish_xy()
    top_parts[3].start_z()
    top_parts[3].finish_z()
    below = descend(0)
    next_parts[0][
        next_.margins[0] : next_.margins[0] + next_.block[0], 0 : next_.block[1], 0:LANES
    ] = below
    next_parts[3].start_xy()
    top_parts[4].start_xy()
    next_parts[3].finish_xy()
    next_parts[3].start_z()
    next_parts[3].finish_z()
    below = descend(1)

    length = tuple(size // 2 for size in next_.block)
    per = LANES // length[2]
    packed = jnp.zeros((8, LANES), F32)
    for plane in range(length[0]):
        moved = below[plane]
        if plane // per:
            moved = pltpu.roll(moved, length[1] * (plane // per), 0)
        if plane % per:
            moved = pltpu.roll(moved, length[2] * (plane % per), 1)
        packed = packed + moved
    own[...] = packed
    slots[me] = packed

    def send(number):
        target, other = peer(number)
        return pltpu.make_async_remote_copy(
            src_ref=own,
            dst_ref=slots.at[me],
            send_sem=sent.at[other],
            recv_sem=got.at[me],
            device_id=target,
            device_id_type=pl.DeviceIdType.MESH,
        )

    def start_send(number, carry):
        send(number).start()
        return carry

    lax.fori_loop(1, total, start_send, 0)
    next_parts[4].start_xy()
    top_parts[4].finish_xy()
    top_parts[4].start_z()
    next_parts[4].finish_xy()
    next_parts[4].start_z()

    def finish_send(number, carry):
        target, other = peer(number)
        copy = pltpu.make_async_remote_copy(
            src_ref=own,
            dst_ref=slots.at[other],
            send_sem=sent.at[other],
            recv_sem=got.at[other],
            device_id=target,
            device_id_type=pl.DeviceIdType.MESH,
        )
        copy.wait_recv()
        copy.wait_send()
        return carry

    lax.fori_loop(1, total, finish_send, 0)

    coarse_source, coarse_field = whole_refs[0]
    lane = iota((8, LANES), 1)

    def place_x(which, carry):
        for second in range(counts[1]):
            base = (which * counts[1] + second) * counts[2]
            tiles = [slots[base + third] for third in range(counts[2])]
            for spot in range(per):
                value = jnp.zeros((8, LANES), F32)
                for third in range(counts[2]):
                    shift = (length[2] * (third - spot)) % LANES
                    moved = pltpu.roll(tiles[third], shift, 1) if shift else tiles[third]
                    value = jnp.where(lane // length[2] == third, moved, value)
                for group in range(8 // length[1]):
                    plane = which * length[0] + group * per + spot
                    coarse_source[plane, second * length[1] : (second + 1) * length[1], :] = value[
                        group * length[1] : (group + 1) * length[1]
                    ]
        return carry

    lax.fori_loop(0, counts[0], place_x, 0)
    solve_whole(levels, whole_refs, pairs, 0)

    def one_hot(shape, dim, fine, fine_length, fine_margin, origin, wrap):
        index = iota(shape, dim)
        spot = local_of(index, fine_length, fine_margin, fine)
        cell = jnp.where(spot >= 0, lax.div(spot, 2), -lax.div(1 - spot, 2)) + origin
        if wrap is not None:
            cell = jnp.where(cell < 0, cell + wrap, cell)
        used = (index < fine_length + fine_margin) | (index >= fine - fine_margin)
        return jnp.where((iota(shape, 1 - dim) == cell) & used, 1.0, 0.0).astype(F32)

    coarse = levels[0]
    rows_to = one_hot(
        (next_.rows, coarse.rows), 0, next_.rows, next_.block[1], next_.margins[1],
        place[1] * length[1], None,
    )
    lanes_to = one_hot(
        (LANES, next_.lanes), 1, next_.lanes, next_.block[2], next_.margins[2],
        place[2] * length[2], None,
    )
    reach = next_.planes // 2

    def plane_of_whole(spot):
        plane = place[0] * length[0] + spot - next_.margins[0] // 2
        return coarse_field[1 + jnp.clip(plane, 0, coarse.shape[0] - 1)]

    next_parts[4].finish_z()
    ascend(1, plane_of_whole, rows_to, lanes_to, reach)

    rows_to = one_hot(
        (top.rows, next_.rows), 0, top.rows, top.block[1], top.margins[1], 0, next_.rows
    )
    lanes_to = one_hot(
        (LANES, top.lanes), 1, top.lanes, top.block[2], top.margins[2], 0, next_.lanes
    )
    shift = next_.margins[0] - top.margins[0] // 2
    top_parts[4].finish_z()
    ascend(0, lambda spot: next_parts[1][1 + spot + shift], rows_to, lanes_to, top.planes // 2)
    potential[...] = top_parts[1][
        1 + top.margins[0] : 1 + top.margins[0] + top.block[0], 0 : top.block[1], 0 : top.block[2]
    ]
    for part in parts:
        part[3].drain()
        part[4].drain()


def flat_scratch(entries):
    out = []
    for entry in entries:
        out.extend(flat_scratch(entry) if isinstance(entry, (list, tuple)) else [entry])
    return out


def on_device(counts, density):
    block = density.shape
    half_block = tuple(size // 2 for size in block)
    splits = [
        Split(block, (4, 4, 4), counts),
        Split(half_block, (6, 8, 8), counts),
    ]
    size = tuple(block[which] * counts[which] // 4 for which in range(3))
    levels = []
    for number in range(2, LEVELS):
        levels.append(Whole(size))
        size = tuple(max(part // 2, 1) for part in size)
    total = counts[0] * counts[1] * counts[2]
    pair_planes = max(block[0] // 2, levels[0].shape[0])
    pair_rows = max(block[1], levels[0].rows, 16)
    scratch = [level.scratch() for level in splits] + [level.scratch() for level in levels]
    scratch = flat_scratch(scratch) + [
        pltpu.VMEM((pair_planes, pair_rows, LANES), F32),
        pltpu.VMEM((max(level.planes // 2 for level in splits), splits[0].rows, LANES), F32),
        pltpu.VMEM((8, LANES), F32),
        pltpu.VMEM((total, 8, LANES), F32),
        pltpu.SemaphoreType.DMA((total,)),
        pltpu.SemaphoreType.DMA((total,)),
    ]
    return pl.pallas_call(
        functools.partial(kernel, splits, levels, counts),
        out_shape=jax.ShapeDtypeStruct(block, F32),
        in_specs=[pl.BlockSpec(memory_space=pltpu.VMEM)],
        out_specs=pl.BlockSpec(memory_space=pltpu.VMEM),
        scratch_shapes=scratch,
        compiler_params=pltpu.CompilerParams(
            collective_id=0, has_side_effects=True, vmem_limit_bytes=48 * 1024 * 1024
        ),
    )(density)


def solution(mesh):
    counts = tuple(mesh.shape[axis] for axis in AXES)
    return jax.shard_map(
        functools.partial(on_device, counts),
        mesh=mesh,
        in_specs=(P("gx", "gy", "gz"),),
        out_specs=P("gx", "gy", "gz"),
        check_vma=False,
    )
```
